32 devices in a mesh: batch: 8 (over z, y), cols: 2 (over core), ens: 2 (over x).
Axes of the slice: x: 2, y: 2, z: 4, core: 2. Of those that a mesh axis runs over, the one named last changes fastest.
Arguments:
- slope_up: float32 [16, 1280, 5120], P(('ens', 'batch'), None, 'cols'), parts along dimension 0, may hold values from -0.875 to 0.875
- slope_down: float32 [16, 5120, 1280], P(('ens', 'batch'), 'cols'), parts along dimension 0, may hold values from -0.875 to 0.875
- slope_norm: float32 [16, 1280], P(('ens', 'batch')), parts along dimension 0, may hold values from -8 to 8
- slope_bias: float32 [16, 1280], P(('ens', 'batch')), parts along dimension 0, may hold values from -8 to 8
- param_up: float32 [2560, 5120], P(('ens', 'batch'), 'cols'), parts along dimension 0, may hold values from -0.25 to 0.25
- param_down: float32 [10240, 1280], P(('ens', 'cols'), 'batch'), parts along dimension 0, may hold values from -0.125 to 0.125
- param_norm: float32 [2560], P(('ens', 'batch')), parts along dimension 0, may hold values from 0.25 to 1.75
- param_bias: float32 [2560], P(('ens', 'batch')), parts along dimension 0, may hold values from -3 to 3
Outputs:
- half_up: bfloat16 [2560, 5120], P('ens', 'cols'), parts along dimension 0
- half_down: bfloat16 [10240, 1280], P(('ens', 'cols')), parts along dimension 0
- half_norm: bfloat16 [2560], P('ens'), parts along dimension 0
- half_bias: bfloat16 [2560], P('ens'), parts along dimension 0
- next_up: float32 [2560, 5120], P(('ens', 'batch'), 'cols'), parts along dimension 0
- next_down: float32 [10240, 1280], P(('ens', 'cols'), 'batch'), parts along dimension 0
- next_norm: float32 [2560], P(('ens', 'batch')), parts along dimension 0
- next_bias: float32 [2560], P(('ens', 'batch')), parts along dimension 0
The draws below stay inside these ranges and needn't reach their ends.
There are 2 independent parts, one for each index of `ens`. The reference program is written for one: setup_inputs(seed, part) draws one part's arguments, and reference() takes and returns one part's arrays. A program takes and returns all parts, laid end to end along the dimension named above; each array names one. Nothing has to cross between parts.
All inputs are finite; a program needn't handle non-finite values.
Results may differ from the reference program's by a relative error of at most 0.008.
Values may be sent and summed in bfloat16 or wider, within the bound.
A program may use at most 128 MiB of HBM per device.

```python
import jax
import jax.numpy as jnp
from jax import lax

WIDTH = 1280
INNER = 5120
REPLICAS = 8


def spiked(values, rng, source, target, shards_of, factor):
    owner, partner = [(jnp.arange(values.shape[position]) // (values.shape[position] // shards_of)).reshape([-1 if axis == position else 1 for axis in range(values.ndim)]) for position in (source, target)]
    chosen = jax.random.permutation(rng, shards_of)[partner]
    strong = (owner == chosen) | (owner == (partner + shards_of // 2) % shards_of)
    return jnp.where(strong, factor * values, values)


def block_levels(rng, dims, shards, low, high):
    loudness = 1.0
    for dim, blocks in shards:
        steps = jax.random.uniform(jax.random.fold_in(jax.random.fold_in(rng, 6), dim), (blocks,), jnp.float32, low / len(shards), high / len(shards))
        loudness = loudness * jnp.repeat(jnp.exp(steps), dims[dim] // blocks).reshape((-1,) + (1,) * (len(dims) - 1 - dim))
    return loudness


def bell_draw(key, dims, width, limit, shards=(), dtype=jnp.bfloat16):
    level = block_levels(key, dims, shards, -0.22, 0.18) if shards else 1.0
    drawn = jax.random.normal(key, dims, jnp.float32) * width * level
    return jnp.minimum(jnp.maximum(drawn, -limit), limit).astype(dtype)


def gaussian_with(key, extent, spread, most, shards, heavy, dtype=jnp.bfloat16):
    result = spread * jax.random.normal(key, extent, jnp.float32)
    if shards:
        result = result * block_levels(key, extent, shards, -0.22, 0.18)
    return jnp.clip(spiked(result, jax.random.fold_in(key, 3), *heavy), -most, most).astype(dtype)


def setup_inputs(seed: int = 0, part: int = 0) -> dict:
    streams_of = jax.random.split(jax.random.key(seed), 9)
    part_keys = jax.random.split(jax.random.fold_in(streams_of[8], part), 9)
    return {
        "slope_up": gaussian_with(part_keys[0], (REPLICAS, WIDTH, INNER), 0.1, 0.875, ((0, 8), (2, 2)), (0, 1, 8, 2.0), jnp.float32),
        "slope_down": gaussian_with(part_keys[1], (REPLICAS, INNER, WIDTH), 0.1, 0.875, ((0, 8), (1, 2)), (0, 2, 8, 2.0), jnp.float32),
        "slope_norm": gaussian_with(part_keys[2], (REPLICAS, WIDTH), 1.0, 8.0, ((0, 8),), (0, 1, 8, 2.0), jnp.float32),
        "slope_bias": gaussian_with(part_keys[3], (REPLICAS, WIDTH), 1.0, 8.0, ((0, 8),), (0, 1, 8, 2.0), jnp.float32),
        "param_up": gaussian_with(part_keys[4], (WIDTH, INNER), WIDTH ** -0.5, 0.25, ((0, 8), (1, 2)), (1, 0, 8, 2.0), jnp.float32),
        "param_down": gaussian_with(part_keys[5], (INNER, WIDTH), INNER ** -0.5, 0.125, ((0, 2), (1, 8)), (0, 1, 8, 2.0), jnp.float32),
        "param_norm": jnp.clip(1.0 + 0.15 * jax.random.normal(part_keys[6], (WIDTH,), jnp.float32), 0.25, 1.75),
        "param_bias": bell_draw(part_keys[7], (WIDTH,), 0.5, 3.0, ((0, 8),), jnp.float32),
    }


learn_rate = 0.4

def reference(slope_up, slope_down, slope_norm, slope_bias, param_up, param_down, param_norm, param_bias):
    mean_up = lax.optimization_barrier(jnp.sum(slope_up.astype(jnp.float32), axis=0)) * REPLICAS ** (-0.5)
    mean_down = lax.optimization_barrier(jnp.sum(slope_down.astype(jnp.float32), axis=0)) * REPLICAS ** (-0.5)
    mean_norm = lax.optimization_barrier(jnp.sum(slope_norm.astype(jnp.float32), axis=0)) * REPLICAS ** (-0.5)
    mean_bias = lax.optimization_barrier(jnp.sum(slope_bias.astype(jnp.float32), axis=0)) * REPLICAS ** (-0.5)
    ratio_up = jnp.sqrt(lax.optimization_barrier(jnp.sum(param_up * param_up, axis=1, keepdims=True))) * lax.rsqrt(lax.optimization_barrier(jnp.sum(mean_up * mean_up, axis=1, keepdims=True)) + 1e-06)
    mean_up = mean_up * ratio_up
    ratio_down = jnp.sqrt(lax.optimization_barrier(jnp.sum(param_down * param_down, axis=0, keepdims=True))) * lax.rsqrt(lax.optimization_barrier(jnp.sum(mean_down * mean_down, axis=0, keepdims=True)) + 1e-06)
    mean_down = mean_down * ratio_down
    next_up = param_up - learn_rate * mean_up
    next_down = param_down - learn_rate * mean_down
    next_norm = param_norm - learn_rate * mean_norm
    next_bias = param_bias - learn_rate * mean_bias
    half_up = next_up.astype(jnp.bfloat16)
    half_down = next_down.astype(jnp.bfloat16)
    half_norm = next_norm.astype(jnp.bfloat16)
    half_bias = next_bias.astype(jnp.bfloat16)
    return (half_up, half_down, half_norm, half_bias, next_up, next_down, next_norm, next_bias)
```

```python
import functools

import jax
import jax.numpy as jnp
from jax import lax
from jax.experimental import pallas as pl
from jax.experimental.pallas import tpu as pltpu
from jax.sharding import PartitionSpec as P

learn_rate = 0.4
MESH = pl.DeviceIdType.MESH
R = 16
LANE = 128
F32, BF16 = jnp.float32, jnp.bfloat16


def kernel(
    n,
    m,
    LA,
    up_ref,
    down_ref,
    pup_ref,
    pdown_ref,
    vec_ref,
    half_ref,
    next_ref,
    sums_ref,
    stage,
    XA,
    XB,
    RYA,
    RYB,
    RZA,
    RZB,
    NX,
    PR,
    SQ,
    GA,
    GB,
    VG,
    up_sem,
    down_sem,
    par_sem,
    out_sem,
    send,
    recv,
    sq_send,
    sq_recv,
    v_send,
    v_recv,
):
    Z = n // 2
    C = NX.shape[0]
    CH = C // 2
    L = NX.shape[2]
    me = lax.axis_index("batch")
    core = lax.axis_index("cols")
    z = me // 2
    y = me % 2
    other = z * 2 + 1 - y
    rate = n ** (-0.5)

    def load_up(c):
        return pltpu.make_async_copy(up_ref.at[:, :, c], stage.at[c % 2], up_sem.at[c % 2])

    def load_down(c):
        k = c - CH
        return [
            pltpu.make_async_copy(
                down_ref.at[:, 0, k, :, pl.ds(0, LA)], XA.at[c, 0], down_sem.at[0, k]
            ),
            pltpu.make_async_copy(
                down_ref.at[:, 1, k, :, pl.ds(0, LA)], XA.at[c, 1], down_sem.at[1, k]
            ),
            pltpu.make_async_copy(
                down_ref.at[:, :, k, :, pl.ds(LA, L - LA)], XB.at[c], down_sem.at[2, k]
            ),
        ]

    def load_params():
        return [
            pltpu.make_async_copy(pup_ref, PR.at[pl.ds(0, CH)], par_sem.at[0]),
            pltpu.make_async_copy(pdown_ref, PR.at[pl.ds(CH, CH)], par_sem.at[1]),
        ]

    load_up(0).start()
    for d in load_params():
        d.start()

    @pl.loop(CH, C)
    def _(c):
        for d in load_down(c):
            d.start()

    barrier = pltpu.get_barrier_semaphore()
    for o in range(1, n):
        pl.semaphore_signal(
            barrier, inc=1, device_id={"batch": (me + o) % n}, device_id_type=MESH
        )
    for o in range(1, m):
        pl.semaphore_signal(
            barrier, inc=1, device_id={"cols": (core + o) % m}, device_id_type=MESH
        )
    pl.semaphore_wait(barrier, n - 1 + m - 1)

    def remote(src, dst, kind, c, to):
        return pltpu.make_async_remote_copy(
            src_ref=src,
            dst_ref=dst,
            send_sem=send.at[kind, c],
            recv_sem=recv.at[kind, c],
            device_id={"batch": to},
            device_id_type=MESH,
        )

    def vec_copy(o):
        return pltpu.make_async_remote_copy(
            src_ref=vec_ref,
            dst_ref=VG.at[o - 1],
            send_sem=v_send.at[o - 1],
            recv_sem=v_recv.at[o - 1],
            device_id={"batch": (me + o) % n},
            device_id_type=MESH,
        )

    for o in range(1, n):
        vec_copy(o).start()

    def sq_copy(c, o):
        return pltpu.make_async_remote_copy(
            src_ref=SQ.at[c, 0],
            dst_ref=SQ.at[c, o],
            send_sem=sq_send.at[o - 1, c],
            recv_sem=sq_recv.at[o - 1, c],
            device_id={"cols": (core + o) % m},
            device_id_type=MESH,
        )

    YA, YB, RA, LFA, RB, LFB, GYA, GYB, GRA, GLA, GRB, GLB = range(12)

    def ya(c):
        return remote(XA.at[c, 1 - y], RYA.at[c], YA, c, other)

    def yb(c):
        return remote(XB.at[c, z, 1 - y], RYB.at[c], YB, c, other)

    def gya(c):
        return remote(GA.at[c, y], GA.at[c, y], GYA, c, other)

    def gya_in(c):
        return remote(GA.at[c, 1 - y], GA.at[c, 1 - y], GYA, c, other)

    def gyb(c):
        return remote(GB.at[c, z, y], GB.at[c, z, y], GYB, c, other)

    def gyb_in(c):
        return remote(GB.at[c, z, 1 - y], GB.at[c, z, 1 - y], GYB, c, other)

    def x_ref(first, c):
        return XA.at[c, y] if first else XB.at[c]

    def sum_right(first, c, k):
        rz = RZA if first else RZB
        return remote(
            x_ref(first, c).at[pl.ds(k + 1, Z - 1 - k)],
            rz.at[c, pl.ds(k + 2, Z - 1 - k)],
            RA if first else RB,
            c,
            jnp.minimum(me + 2, n - 1),
        )

    def sum_left(first, c, k):
        rz = RZA if first else RZB
        return remote(
            x_ref(first, c).at[pl.ds(0, k)],
            rz.at[c, pl.ds(0, k)],
            LFA if first else LFB,
            c,
            jnp.maximum(me - 2, 0),
        )

    def add(first, c, lo, count, slot):
        rz = RZA if first else RZB
        for d in range(count):
            if first:
                XA[c, y, lo + d] = (
                    XA[c, y, lo + d].astype(F32) + rz[c, slot + d].astype(F32)
                ).astype(BF16)
            else:
                XB[c, lo + d] = (
                    XB[c, lo + d].astype(F32) + rz[c, slot + d].astype(F32)
                ).astype(BF16)

    def reduce_step(first, t):
        for k in range(Z):

            @pl.when((z == k) & (t - k >= 0) & (t - k < C))
            def _():
                c = t - k
                if k > 0:
                    sum_right(first, c, k - 1).wait_recv()
                    add(first, c, k, Z - k, k + 1)
                if k < Z - 1:
                    sum_right(first, c, k).start()

            q = Z - 1 - k

            @pl.when((z == k) & (t - q >= 0) & (t - q < C))
            def _():
                c = t - q
                if k < Z - 1:
                    sum_left(first, c, k + 1).wait_recv()
                    add(first, c, 0, k + 1, 0)
                if k > 0:
                    sum_left(first, c, k).start()

    def g_ref(first, c):
        return GA.at[c, y] if first else GB.at[c]

    def gather_right(first, c, k):
        ref = g_ref(first, c).at[pl.ds(0, k + 1)]
        return remote(ref, ref, GRA if first else GRB, c, jnp.minimum(me + 2, n - 1))

    def gather_left(first, c, k):
        ref = g_ref(first, c).at[pl.ds(k, Z - k)]
        return remote(ref, ref, GLA if first else GLB, c, jnp.maximum(me - 2, 0))

    def gather_step(first, t):
        for k in range(Z):

            @pl.when((z == k) & (t - k >= 0) & (t - k < C))
            def _():
                c = t - k
                if k > 0:
                    gather_right(first, c, k - 1).wait_recv()
                if k < Z - 1:
                    gather_right(first, c, k).start()

            q = Z - 1 - k

            @pl.when((z == k) & (t - q >= 0) & (t - q < C))
            def _():
                c = t - q
                if k < Z - 1:
                    gather_left(first, c, k + 1).wait_recv()
                if k > 0:
                    gather_left(first, c, k).start()

    def outs(c):
        w = c // CH
        k = c % CH
        return [
            pltpu.make_async_copy(
                GA.at[c, 0], half_ref.at[w, :, 0, k, :, pl.ds(0, LA)], out_sem.at[0, c]
            ),
            pltpu.make_async_copy(
                GA.at[c, 1], half_ref.at[w, :, 1, k, :, pl.ds(0, LA)], out_sem.at[1, c]
            ),
            pltpu.make_async_copy(
                GB.at[c], half_ref.at[w, :, :, k, :, pl.ds(LA, L - LA)], out_sem.at[2, c]
            ),
        ]

    def next_out(c):
        return pltpu.make_async_copy(NX.at[c], next_ref.at[c], out_sem.at[3, c])

    def lanes(x):
        s = x[:, :LANE] * x[:, :LANE]
        for i in range(1, L // LANE):
            part = x[:, i * LANE : (i + 1) * LANE]
            s = s + part * part
        return s

    def when_chunk(c):
        return pl.when((c >= 0) & (c < C))

    @pl.loop(0, C + 2 * Z + 2)
    def _(t):
        @pl.when(t + 1 < CH)
        def _():
            load_up(t + 1).start()

        @pl.when(t < CH)
        def _():
            load_up(t).wait()
            for d in range(Z):
                for v in range(2):
                    XA[t, v, d] = stage[t % 2, d, v, :, :LA].astype(BF16)
                    XB[t, d, v] = stage[t % 2, d, v, :, LA:].astype(BF16)

        @pl.when((t >= CH) & (t < C))
        def _():
            for d in load_down(t):
                d.wait()

        @pl.when(t < C)
        def _():
            ya(t).start()

        reduce_step(False, t)
        s = t - 1

        @when_chunk(s)
        def _():
            ya(s).wait_recv()
            for d in range(Z):
                XA[s, y, d] = (XA[s, y, d].astype(F32) + RYA[s, d].astype(F32)).astype(BF16)

        reduce_step(True, s)
        b = t - (Z - 1)

        @when_chunk(b)
        def _():
            yb(b).start()

        f = t - Z

        @pl.when(f == 0)
        def _():
            for d in load_params():
                d.wait()

        @when_chunk(f)
        def _():
            yb(f).wait_recv()
            NX[f, :, :LA] = XA[f, y, z].astype(F32) * rate
            NX[f, :, LA:] = (XB[f, z, y].astype(F32) + RYB[f].astype(F32)) * rate
            SQ[f, 0, 0] = lanes(NX[f])
            SQ[f, 0, 1] = lanes(PR[f])
            for o in range(1, m):
                sq_copy(f, o).start()

        u = t - Z - 1

        @when_chunk(u)
        def _():
            for o in range(1, m):
                sq_copy(u, o).wait_recv()
            g = SQ[u, 0, 0]
            p = SQ[u, 0, 1]
            for o in range(1, m):
                g = g + SQ[u, o, 0]
                p = p + SQ[u, o, 1]
            g = jnp.sum(g, axis=1, keepdims=True)
            p = jnp.sum(p, axis=1, keepdims=True)
            scale = learn_rate * (jnp.sqrt(p) * lax.rsqrt(g + 1e-06))
            new = PR[u] - NX[u] * scale
            NX[u] = new
            half = new.astype(BF16)
            GA[u, y, z] = half[:, :LA]
            GB[u, z, y] = half[:, LA:]
            gyb(u).start()
            next_out(u).start()

        gather_step(True, u)

        @when_chunk(u - 1)
        def _():
            gyb_in(u - 1).wait_recv()

        gather_step(False, u - 1)

        @when_chunk(u - (Z - 1))
        def _():
            gya(u - (Z - 1)).start()

        e = u - Z

        @when_chunk(e)
        def _():
            gya_in(e).wait_recv()
            for d in outs(e):
                d.start()

    total = vec_ref[...]
    for o in range(1, n):
        vec_copy(o).wait()
        total = total + VG[o - 1]
    sums_ref[...] = total

    @pl.loop(0, C)
    def _(c):
        for d in outs(c):
            d.wait()
        next_out(c).wait()
        for d in (ya(c), yb(c), gya(c), gyb(c)):
            d.wait_send()
        for o in range(1, m):
            sq_copy(c, o).wait_send()
        for k in range(Z):

            @pl.when(z == k)
            def _():
                for first in (True, False):
                    if k < Z - 1:
                        sum_right(first, c, k).wait_send()
                        gather_right(first, c, k).wait_send()
                    if k > 0:
                        sum_left(first, c, k).wait_send()
                        gather_left(first, c, k).wait_send()


def on_device(
    slope_up, slope_down, slope_norm, slope_bias, param_up, param_down, param_norm, param_bias
):
    n = lax.axis_size("batch")
    m = lax.axis_size("cols")
    Z = n // 2
    rows, L = param_up.shape
    CH = rows // R
    C = 2 * CH
    LA = max(1, round(0.6 * L / LANE)) * LANE
    LB = L - LA
    width = slope_norm.shape[1]
    place = lax.axis_index("batch")
    up = slope_up[0].reshape(Z, 2, CH, R, L)
    down = slope_down[0].astype(BF16).T.reshape(Z, 2, CH, R, L)
    pup = param_up.reshape(CH, R, L)
    pdown = param_down.T.reshape(CH, R, L)
    mine = lax.dynamic_update_slice(
        jnp.zeros((2, width), F32), jnp.stack([param_norm, param_bias]), (0, place * rows)
    )
    vec = jnp.concatenate([slope_norm, slope_bias, mine], axis=0).reshape(8, width // 2)
    kinds = 12
    hbm = pl.BlockSpec(memory_space=pl.ANY)
    vmem = pl.BlockSpec(memory_space=pltpu.VMEM)
    half, new, sums = pl.pallas_call(
        functools.partial(kernel, n, m, LA),
        out_shape=(
            jax.ShapeDtypeStruct((2, Z, 2, CH, R, L), BF16),
            jax.ShapeDtypeStruct((C, R, L), F32),
            jax.ShapeDtypeStruct(vec.shape, F32),
        ),
        in_specs=[hbm, hbm, hbm, hbm, vmem],
        out_specs=(hbm, hbm, vmem),
        scratch_shapes=[
            pltpu.VMEM((2, Z, 2, R, L), F32),
            pltpu.VMEM((C, 2, Z, R, LA), BF16),
            pltpu.VMEM((C, Z, 2, R, LB), BF16),
            pltpu.VMEM((C, Z, R, LA), BF16),
            pltpu.VMEM((C, R, LB), BF16),
            pltpu.VMEM((C, Z + 1, R, LA), BF16),
            pltpu.VMEM((C, Z + 1, 2, R, LB), BF16),
            pltpu.VMEM((C, R, L), F32),
            pltpu.VMEM((C, R, L), F32),
            pltpu.VMEM((C, m, 2, R, LANE), F32),
            pltpu.VMEM((C, 2, Z, R, LA), BF16),
            pltpu.VMEM((C, Z, 2, R, LB), BF16),
            pltpu.VMEM((n - 1,) + vec.shape, F32),
            pltpu.SemaphoreType.DMA((2,)),
            pltpu.SemaphoreType.DMA((3, CH)),
            pltpu.SemaphoreType.DMA((2,)),
            pltpu.SemaphoreType.DMA((4, C)),
            pltpu.SemaphoreType.DMA((kinds, C)),
            pltpu.SemaphoreType.DMA((kinds, C)),
            pltpu.SemaphoreType.DMA((m - 1, C)),
            pltpu.SemaphoreType.DMA((m - 1, C)),
            pltpu.SemaphoreType.DMA((n - 1,)),
            pltpu.SemaphoreType.DMA((n - 1,)),
        ],
        compiler_params=pltpu.CompilerParams(
            collective_id=0, has_side_effects=True, vmem_limit_bytes=67043328
        ),
    )(up, down, pup, pdown, vec)
    half_up = half[0].reshape(n * rows, L)
    half_down = half[1].reshape(n * rows, L).T
    next_up = new[:CH].reshape(rows, L)
    next_down = new[CH:].reshape(rows, L).T
    sums = sums.reshape(4, width)
    whole = sums[2:] - learn_rate * (sums[:2] * n ** (-0.5))
    own = lax.dynamic_slice_in_dim(whole, place * rows, rows, axis=1)
    halves = whole.astype(BF16)
    return (half_up, half_down, halves[0], halves[1], next_up, next_down, own[0], own[1])


def solution(mesh):
    return jax.shard_map(
        on_device,
        mesh=mesh,
        in_specs=(
            P(("ens", "batch"), None, "cols"),
            P(("ens", "batch"), "cols", None),
            P(("ens", "batch"), None),
            P(("ens", "batch"), None),
            P(("ens", "batch"), "cols"),
            P(("ens", "cols"), "batch"),
            P(("ens", "batch")),
            P(("ens", "batch")),
        ),
        out_specs=(
            P("ens", "cols"),
            P(("ens", "cols"), None),
            P("ens"),
            P("ens"),
            P(("ens", "batch"), "cols"),
            P(("ens", "cols"), "batch"),
            P(("ens", "batch")),
            P(("ens", "batch")),
        ),
        check_vma=False,
    )
```

```python
import functools

import jax
import jax.numpy as jnp
from jax import lax
from jax.experimental import pallas as pl
from jax.experimental.pallas import tpu as pltpu
from jax.sharding import PartitionSpec as P

learn_rate = 0.4
MESH = pl.DeviceIdType.MESH
R = 8
LANE = 128
SPLIT = 0.6
F32, BF16 = jnp.float32, jnp.bfloat16


def kernel(
    n,
    m,
    LA,
    up_ref,
    down_ref,
    pup_ref,
    pdown_ref,
    vec_ref,
    half_up_ref,
    half_down_ref,
    next_ref,
    sums_ref,
    stage,
    turn,
    XA,
    XB,
    RYA,
    RYB,
    RZA,
    RZB,
    NX,
    PR,
    SQ,
    GA,
    GB,
    VG,
    up_sem,
    down_sem,
    par_sem,
    out_sem,
    send,
    recv,
    sq_send,
    sq_recv,
    v_send,
    v_recv,
):
    Z = n // 2
    C = NX.shape[0]
    CH = C // 2
    L = NX.shape[2]
    me = lax.axis_index("batch")
    core = lax.axis_index("cols")
    z = me // 2
    y = me % 2
    other = z * 2 + 1 - y
    rate = n ** (-0.5)

    def load_up(c):
        return pltpu.make_async_copy(up_ref.at[:, :, c], stage.at[c % 2], up_sem.at[c % 2])

    blocks = L // LANE
    share = -(-blocks // CH)

    def load_down(b):
        return pltpu.make_async_copy(
            down_ref.at[pl.ds(b * LANE, LANE)], turn.at[b % 2], down_sem.at[b % 2]
        )

    def turn_block(b):
        def pieces(store):
            for j in range(n * CH * R // LANE):
                tile = turn[b % 2, :, j * LANE : (j + 1) * LANE].T
                for i in range(LANE // R):
                    piece = j * (LANE // R) + i
                    d, k = piece // CH, piece % CH
                    store(d // 2, d % 2, CH + k, tile[i * R : (i + 1) * R].astype(BF16))

        @pl.when(b * LANE < LA)
        def _():
            at = pl.ds(pl.multiple_of(b * LANE, LANE), LANE)

            def store(d, v, c, x):
                XA[c, v, d, :, at] = x

            pieces(store)

        @pl.when(b * LANE >= LA)
        def _():
            at = pl.ds(pl.multiple_of(b * LANE - LA, LANE), LANE)

            def store(d, v, c, x):
                XB[c, d, v, :, at] = x

            pieces(store)

    def load_params():
        return [
            pltpu.make_async_copy(pup_ref, PR.at[pl.ds(0, CH)], par_sem.at[0]),
            pltpu.make_async_copy(pdown_ref, PR.at[pl.ds(CH, CH)], par_sem.at[1]),
        ]

    load_up(0).start()
    for d in load_params():
        d.start()

    load_down(0).start()

    barrier = pltpu.get_barrier_semaphore()
    for o in range(1, n):
        pl.semaphore_signal(
            barrier, inc=1, device_id={"batch": (me + o) % n}, device_id_type=MESH
        )
    for o in range(1, m):
        pl.semaphore_signal(
            barrier, inc=1, device_id={"cols": (core + o) % m}, device_id_type=MESH
        )
    pl.semaphore_wait(barrier, n - 1 + m - 1)

    def remote(src, dst, kind, c, to):
        return pltpu.make_async_remote_copy(
            src_ref=src,
            dst_ref=dst,
            send_sem=send.at[kind, c],
            recv_sem=recv.at[kind, c],
            device_id={"batch": to},
            device_id_type=MESH,
        )

    def vec_copy(o):
        return pltpu.make_async_remote_copy(
            src_ref=vec_ref,
            dst_ref=VG.at[o - 1],
            send_sem=v_send.at[o - 1],
            recv_sem=v_recv.at[o - 1],
            device_id={"batch": (me + o) % n},
            device_id_type=MESH,
        )

    for o in range(1, n):
        vec_copy(o).start()

    def sq_copy(c, o):
        return pltpu.make_async_remote_copy(
            src_ref=SQ.at[c, 0],
            dst_ref=SQ.at[c, o],
            send_sem=sq_send.at[o - 1, c],
            recv_sem=sq_recv.at[o - 1, c],
            device_id={"cols": (core + o) % m},
            device_id_type=MESH,
        )

    YA, YB, RA, LFA, RB, LFB, GYA, GYB, GRA, GLA, GRB, GLB = range(12)

    def ya(c):
        return remote(XA.at[c, 1 - y], RYA.at[c], YA, c, other)

    def yb(c):
        return remote(XB.at[c, z, 1 - y], RYB.at[c], YB, c, other)

    def gya(c):
        return remote(GA.at[c, y], GA.at[c, y], GYA, c, other)

    def gya_in(c):
        return remote(GA.at[c, 1 - y], GA.at[c, 1 - y], GYA, c, other)

    def gyb(c):
        return remote(GB.at[c, z, y], GB.at[c, z, y], GYB, c, other)

    def gyb_in(c):
        return remote(GB.at[c, z, 1 - y], GB.at[c, z, 1 - y], GYB, c, other)

    def x_ref(first, c):
        return XA.at[c, y] if first else XB.at[c]

    def sum_right(first, c, k):
        rz = RZA if first else RZB
        return remote(
            x_ref(first, c).at[pl.ds(k + 1, Z - 1 - k)],
            rz.at[c, pl.ds(k + 2, Z - 1 - k)],
            RA if first else RB,
            c,
            jnp.minimum(me + 2, n - 1),
        )

    def sum_left(first, c, k):
        rz = RZA if first else RZB
        return remote(
            x_ref(first, c).at[pl.ds(0, k)],
            rz.at[c, pl.ds(0, k)],
            LFA if first else LFB,
            c,
            jnp.maximum(me - 2, 0),
        )

    def add(first, c, lo, count, slot):
        rz = RZA if first else RZB
        for d in range(count):
            if first:
                XA[c, y, lo + d] = (
                    XA[c, y, lo + d].astype(F32) + rz[c, slot + d].astype(F32)
                ).astype(BF16)
            else:
                XB[c, lo + d] = (
                    XB[c, lo + d].astype(F32) + rz[c, slot + d].astype(F32)
                ).astype(BF16)

    def reduce_step(first, t):
        for k in range(Z):

            @pl.when((z == k) & (t - k >= 0) & (t - k < C))
            def _():
                c = t - k
                if k > 0:
                    sum_right(first, c, k - 1).wait_recv()
                    add(first, c, k, Z - k, k + 1)
                if k < Z - 1:
                    sum_right(first, c, k).start()

            q = Z - 1 - k

            @pl.when((z == k) & (t - q >= 0) & (t - q < C))
            def _():
                c = t - q
                if k < Z - 1:
                    sum_left(first, c, k + 1).wait_recv()
                    add(first, c, 0, k + 1, 0)
                if k > 0:
                    sum_left(first, c, k).start()

    def g_ref(first, c):
        return GA.at[c, y] if first else GB.at[c]

    def gather_right(first, c, k):
        ref = g_ref(first, c).at[pl.ds(0, k + 1)]
        return remote(ref, ref, GRA if first else GRB, c, jnp.minimum(me + 2, n - 1))

    def gather_left(first, c, k):
        ref = g_ref(first, c).at[pl.ds(k, Z - k)]
        return remote(ref, ref, GLA if first else GLB, c, jnp.maximum(me - 2, 0))

    def gather_step(first, t):
        for k in range(Z):

            @pl.when((z == k) & (t - k >= 0) & (t - k < C))
            def _():
                c = t - k
                if k > 0:
                    gather_right(first, c, k - 1).wait_recv()
                if k < Z - 1:
                    gather_right(first, c, k).start()

            q = Z - 1 - k

            @pl.when((z == k) & (t - q >= 0) & (t - q < C))
            def _():
                c = t - q
                if k < Z - 1:
                    gather_left(first, c, k + 1).wait_recv()
                if k > 0:
                    gather_left(first, c, k).start()

    def outs(c, act):
        def each(half_ref, k):
            for d in (
                pltpu.make_async_copy(
                    GA.at[c, 0], half_ref.at[:, 0, k, :, pl.ds(0, LA)], out_sem.at[0, c]
                ),
                pltpu.make_async_copy(
                    GA.at[c, 1], half_ref.at[:, 1, k, :, pl.ds(0, LA)], out_sem.at[1, c]
                ),
                pltpu.make_async_copy(
                    GB.at[c], half_ref.at[:, :, k, :, pl.ds(LA, L - LA)], out_sem.at[2, c]
                ),
            ):
                act(d)

        @pl.when(c < CH)
        def _():
            each(half_up_ref, c)

        @pl.when(c >= CH)
        def _():
            each(half_down_ref, c - CH)

    def next_out(c):
        return pltpu.make_async_copy(NX.at[c], next_ref.at[c], out_sem.at[3, c])

    def lanes(x):
        s = x[:, :LANE] * x[:, :LANE]
        for i in range(1, L // LANE):
            part = x[:, i * LANE : (i + 1) * LANE]
            s = s + part * part
        return s

    def when_chunk(c):
        return pl.when((c >= 0) & (c < C))

    @pl.loop(0, C + 2 * Z + 2)
    def _(t):
        @pl.when(t + 1 < CH)
        def _():
            load_up(t + 1).start()

        @pl.when(t < CH)
        def _():
            load_up(t).wait()
            for d in range(Z):
                for v in range(2):
                    XA[t, v, d] = stage[t % 2, d, v, :, :LA].astype(BF16)
                    XB[t, d, v] = stage[t % 2, d, v, :, LA:].astype(BF16)

        @pl.when(t < C)
        def _():
            ya(t).start()

        for i in range(share):
            b = t * share + i

            @pl.when(b + 1 < blocks)
            def _():
                load_down(b + 1).start()

            @pl.when(b < blocks)
            def _():
                load_down(b).wait()
                turn_block(b)

        reduce_step(False, t)
        s = t - 1

        @when_chunk(s)
        def _():
            ya(s).wait_recv()
            for d in range(Z):
                XA[s, y, d] = (XA[s, y, d].astype(F32) + RYA[s, d].astype(F32)).astype(BF16)

        reduce_step(True, s)
        b = t - (Z - 1)

        @when_chunk(b)
        def _():
            yb(b).start()

        f = t - Z

        @pl.when(f == 0)
        def _():
            for d in load_params():
                d.wait()

        @when_chunk(f)
        def _():
            yb(f).wait_recv()
            NX[f, :, :LA] = XA[f, y, z].astype(F32) * rate
            NX[f, :, LA:] = (XB[f, z, y].astype(F32) + RYB[f].astype(F32)) * rate
            SQ[f, 0, 0] = lanes(NX[f])
            SQ[f, 0, 1] = lanes(PR[f])
            for o in range(1, m):
                sq_copy(f, o).start()

        u = t - Z - 1

        @when_chunk(u)
        def _():
            for o in range(1, m):
                sq_copy(u, o).wait_recv()
            g = SQ[u, 0, 0]
            p = SQ[u, 0, 1]
            for o in range(1, m):
                g = g + SQ[u, o, 0]
                p = p + SQ[u, o, 1]
            g = jnp.sum(g, axis=1, keepdims=True)
            p = jnp.sum(p, axis=1, keepdims=True)
            scale = learn_rate * (jnp.sqrt(p) * lax.rsqrt(g + 1e-06))
            new = PR[u] - NX[u] * scale
            NX[u] = new
            half = new.astype(BF16)
            GA[u, y, z] = half[:, :LA]
            GB[u, z, y] = half[:, LA:]
            gyb(u).start()
            next_out(u).start()

        gather_step(True, u)

        @when_chunk(u - 1)
        def _():
            gyb_in(u - 1).wait_recv()

        gather_step(False, u - 1)

        @when_chunk(u - (Z - 1))
        def _():
            gya(u - (Z - 1)).start()

        e = u - Z

        @when_chunk(e)
        def _():
            gya_in(e).wait_recv()
            outs(e, lambda d: d.start())

    total = vec_ref[...]
    for o in range(1, n):
        vec_copy(o).wait()
        total = total + VG[o - 1]
    sums_ref[...] = total

    @pl.loop(0, C)
    def _(c):
        outs(c, lambda d: d.wait())
        next_out(c).wait()
        for d in (ya(c), yb(c), gya(c), gyb(c)):
            d.wait_send()
        for o in range(1, m):
            sq_copy(c, o).wait_send()
        for k in range(Z):

            @pl.when(z == k)
            def _():
                for first in (True, False):
                    if k < Z - 1:
                        sum_right(first, c, k).wait_send()
                        gather_right(first, c, k).wait_send()
                    if k > 0:
                        sum_left(first, c, k).wait_send()
                        gather_left(first, c, k).wait_send()


def on_device(
    slope_up, slope_down, slope_norm, slope_bias, param_up, param_down, param_norm, param_bias
):
    n = lax.axis_size("batch")
    m = lax.axis_size("cols")
    Z = n // 2
    rows, L = param_up.shape
    CH = rows // R
    C = 2 * CH
    LA = max(1, round(SPLIT * L / LANE)) * LANE
    LB = L - LA
    width = slope_norm.shape[1]
    place = lax.axis_index("batch")
    up = slope_up[0].reshape(Z, 2, CH, R, L)
    down = slope_down[0]
    pup = param_up.reshape(CH, R, L)
    pdown = param_down.T.reshape(CH, R, L)
    mine = lax.dynamic_update_slice(
        jnp.zeros((2, width), F32), jnp.stack([param_norm, param_bias]), (0, place * rows)
    )
    vec = jnp.concatenate([slope_norm, slope_bias, mine], axis=0).reshape(8, width // 2)
    kinds = 12
    hbm = pl.BlockSpec(memory_space=pl.ANY)
    vmem = pl.BlockSpec(memory_space=pltpu.VMEM)
    half_up, half_down, new, sums = pl.pallas_call(
        functools.partial(kernel, n, m, LA),
        out_shape=(
            jax.ShapeDtypeStruct((Z, 2, CH, R, L), BF16),
            jax.ShapeDtypeStruct((Z, 2, CH, R, L), BF16),
            jax.ShapeDtypeStruct((C, R, L), F32),
            jax.ShapeDtypeStruct(vec.shape, F32),
        ),
        in_specs=[hbm, hbm, hbm, hbm, vmem],
        out_specs=(hbm, hbm, hbm, vmem),
        scratch_shapes=[
            pltpu.VMEM((2, Z, 2, R, L), F32),
            pltpu.VMEM((2, LANE, n * rows), F32),
            pltpu.VMEM((C, 2, Z, R, LA), BF16),
            pltpu.VMEM((C, Z, 2, R, LB), BF16),
            pltpu.VMEM((C, Z, R, LA), BF16),
            pltpu.VMEM((C, R, LB), BF16),
            pltpu.VMEM((C, Z + 1, R, LA), BF16),
            pltpu.VMEM((C, Z + 1, 2, R, LB), BF16),
            pltpu.VMEM((C, R, L), F32),
            pltpu.VMEM((C, R, L), F32),
            pltpu.VMEM((C, m, 2, R, LANE), F32),
            pltpu.VMEM((C, 2, Z, R, LA), BF16),
            pltpu.VMEM((C, Z, 2, R, LB), BF16),
            pltpu.VMEM((n - 1,) + vec.shape, F32),
            pltpu.SemaphoreType.DMA((2,)),
            pltpu.SemaphoreType.DMA((2,)),
            pltpu.SemaphoreType.DMA((2,)),
            pltpu.SemaphoreType.DMA((4, C)),
            pltpu.SemaphoreType.DMA((kinds, C)),
            pltpu.SemaphoreType.DMA((kinds, C)),
            pltpu.SemaphoreType.DMA((m - 1, C)),
            pltpu.SemaphoreType.DMA((m - 1, C)),
            pltpu.SemaphoreType.DMA((n - 1,)),
            pltpu.SemaphoreType.DMA((n - 1,)),
        ],
        compiler_params=pltpu.CompilerParams(
            collective_id=0, has_side_effects=True, vmem_limit_bytes=67043328
        ),
    )(up, down, pup, pdown, vec)
    half_up = half_up.reshape(n * rows, L)
    half_down = half_down.reshape(n * rows, L).T
    next_up = new[:CH].reshape(rows, L)
    next_down = new[CH:].reshape(rows, L).T
    sums = sums.reshape(4, width)
    whole = sums[2:] - learn_rate * (sums[:2] * n ** (-0.5))
    own = lax.dynamic_slice_in_dim(whole, place * rows, rows, axis=1)
    halves = whole.astype(BF16)
    return (half_up, half_down, halves[0], halves[1], next_up, next_down, own[0], own[1])


def solution(mesh):
    return jax.shard_map(
        on_device,
        mesh=mesh,
        in_specs=(
            P(("ens", "batch"), None, "cols"),
            P(("ens", "batch"), "cols", None),
            P(("ens", "batch"), None),
            P(("ens", "batch"), None),
            P(("ens", "batch"), "cols"),
            P(("ens", "cols"), "batch"),
            P(("ens", "batch")),
            P(("ens", "batch")),
        ),
        out_specs=(
            P("ens", "cols"),
            P(("ens", "cols"), None),
            P("ens"),
            P("ens"),
            P(("ens", "batch"), "cols"),
            P(("ens", "cols"), "batch"),
            P(("ens", "batch")),
            P(("ens", "batch")),
        ),
        check_vma=False,
    )
```

```python
import functools

import jax
import jax.numpy as jnp
from jax import lax
from jax.experimental import pallas as pl
from jax.experimental.pallas import tpu as pltpu
from jax.sharding import PartitionSpec as P

learn_rate = 0.4
MESH = pl.DeviceIdType.MESH
R = 8
LANE = 128
SPLIT = 0.6
F32, BF16 = jnp.float32, jnp.bfloat16


def kernel(
    n,
    m,
    LA,
    up_ref,
    down_ref,
    pup_ref,
    pdown_ref,
    vec_ref,
    half_up_ref,
    half_down_ref,
    next_up_ref,
    next_down_ref,
    sums_ref,
    stage,
    turn,
    XA,
    XB,
    RYA,
    RYB,
    RZA,
    RZB,
    NX,
    PR,
    SQ,
    GA,
    GB,
    VG,
    up_sem,
    down_sem,
    par_sem,
    out_sem,
    send,
    recv,
    sq_send,
    sq_recv,
    v_send,
    v_recv,
):
    Z = n // 2
    C = NX.shape[0]
    CH = C // 2
    L = NX.shape[2]
    me = lax.axis_index("batch")
    core = lax.axis_index("cols")
    z = me // 2
    y = me % 2
    other = z * 2 + 1 - y
    rate = n ** (-0.5)

    def load_up(c):
        return pltpu.make_async_copy(up_ref.at[:, :, c], stage.at[c % 2], up_sem.at[c % 2])

    blocks = L // LANE
    share = -(-blocks // CH)

    def load_down(b):
        return pltpu.make_async_copy(
            down_ref.at[pl.ds(b * LANE, LANE)], turn.at[b % 2], down_sem.at[b % 2]
        )

    def turn_block(b):
        def pieces(store):
            for j in range(n * CH * R // LANE):
                tile = turn[b % 2, :, j * LANE : (j + 1) * LANE].T
                for i in range(LANE // R):
                    piece = j * (LANE // R) + i
                    d, k = piece // CH, piece % CH
                    store(d // 2, d % 2, CH + k, tile[i * R : (i + 1) * R].astype(BF16))

        @pl.when(b * LANE < LA)
        def _():
            at = pl.ds(pl.multiple_of(b * LANE, LANE), LANE)

            def store(d, v, c, x):
                XA[c, v, d, :, at] = x

            pieces(store)

        @pl.when(b * LANE >= LA)
        def _():
            at = pl.ds(pl.multiple_of(b * LANE - LA, LANE), LANE)

            def store(d, v, c, x):
                XB[c, d, v, :, at] = x

            pieces(store)

    def load_params():
        return [
            pltpu.make_async_copy(pup_ref, PR.at[pl.ds(0, CH)], par_sem.at[0]),
            pltpu.make_async_copy(pdown_ref, PR.at[pl.ds(CH, CH)], par_sem.at[1]),
        ]

    load_up(0).start()
    for d in load_params():
        d.start()

    load_down(0).start()

    barrier = pltpu.get_barrier_semaphore()
    for o in range(1, n):
        pl.semaphore_signal(
            barrier, inc=1, device_id={"batch": (me + o) % n}, device_id_type=MESH
        )
    for o in range(1, m):
        pl.semaphore_signal(
            barrier, inc=1, device_id={"cols": (core + o) % m}, device_id_type=MESH
        )
    pl.semaphore_wait(barrier, n - 1 + m - 1)

    def remote(src, dst, kind, c, to):
        return pltpu.make_async_remote_copy(
            src_ref=src,
            dst_ref=dst,
            send_sem=send.at[kind, c],
            recv_sem=recv.at[kind, c],
            device_id={"batch": to},
            device_id_type=MESH,
        )

    def vec_copy(o):
        return pltpu.make_async_remote_copy(
            src_ref=vec_ref,
            dst_ref=VG.at[o - 1],
            send_sem=v_send.at[o - 1],
            recv_sem=v_recv.at[o - 1],
            device_id={"batch": (me + o) % n},
            device_id_type=MESH,
        )

    for o in range(1, n):
        vec_copy(o).start()

    def sq_copy(c, o):
        return pltpu.make_async_remote_copy(
            src_ref=SQ.at[c, 0],
            dst_ref=SQ.at[c, o],
            send_sem=sq_send.at[o - 1, c],
            recv_sem=sq_recv.at[o - 1, c],
            device_id={"cols": (core + o) % m},
            device_id_type=MESH,
        )

    YA, YB, RA, LFA, RB, LFB, GYA, GYB, GRA, GLA, GRB, GLB = range(12)

    def ya(c):
        return remote(XA.at[c, 1 - y], RYA.at[c], YA, c, other)

    def yb(c):
        return remote(XB.at[c, z, 1 - y], RYB.at[c], YB, c, other)

    def gya(c):
        return remote(GA.at[c, y], GA.at[c, y], GYA, c, other)

    def gya_in(c):
        return remote(GA.at[c, 1 - y], GA.at[c, 1 - y], GYA, c, other)

    def gyb(c):
        return remote(GB.at[c, z, y], GB.at[c, z, y], GYB, c, other)

    def gyb_in(c):
        return remote(GB.at[c, z, 1 - y], GB.at[c, z, 1 - y], GYB, c, other)

    def x_ref(first, c):
        return XA.at[c, y] if first else XB.at[c]

    def sum_right(first, c, k):
        rz = RZA if first else RZB
        return remote(
            x_ref(first, c).at[pl.ds(k + 1, Z - 1 - k)],
            rz.at[c, pl.ds(k + 2, Z - 1 - k)],
            RA if first else RB,
            c,
            jnp.minimum(me + 2, n - 1),
        )

    def sum_left(first, c, k):
        rz = RZA if first else RZB
        return remote(
            x_ref(first, c).at[pl.ds(0, k)],
            rz.at[c, pl.ds(0, k)],
            LFA if first else LFB,
            c,
            jnp.maximum(me - 2, 0),
        )

    def add(first, c, lo, count, slot):
        rz = RZA if first else RZB
        for d in range(count):
            if first:
                XA[c, y, lo + d] = (
                    XA[c, y, lo + d].astype(F32) + rz[c, slot + d].astype(F32)
                ).astype(BF16)
            else:
                XB[c, lo + d] = (
                    XB[c, lo + d].astype(F32) + rz[c, slot + d].astype(F32)
                ).astype(BF16)

    def reduce_step(first, t):
        for k in range(Z):

            @pl.when((z == k) & (t - k >= 0) & (t - k < C))
            def _():
                c = t - k
                if k > 0:
                    sum_right(first, c, k - 1).wait_recv()
                    add(first, c, k, Z - k, k + 1)
                if k < Z - 1:
                    sum_right(first, c, k).start()

            q = Z - 1 - k

            @pl.when((z == k) & (t - q >= 0) & (t - q < C))
            def _():
                c = t - q
                if k < Z - 1:
                    sum_left(first, c, k + 1).wait_recv()
                    add(first, c, 0, k + 1, 0)
                if k > 0:
                    sum_left(first, c, k).start()

    def g_ref(first, c):
        return GA.at[c, y] if first else GB.at[c]

    def gather_right(first, c, k):
        ref = g_ref(first, c).at[pl.ds(0, k + 1)]
        return remote(ref, ref, GRA if first else GRB, c, jnp.minimum(me + 2, n - 1))

    def gather_left(first, c, k):
        ref = g_ref(first, c).at[pl.ds(k, Z - k)]
        return remote(ref, ref, GLA if first else GLB, c, jnp.maximum(me - 2, 0))

    def gather_step(first, t):
        for k in range(Z):

            @pl.when((z == k) & (t - k >= 0) & (t - k < C))
            def _():
                c = t - k
                if k > 0:
                    gather_right(first, c, k - 1).wait_recv()
                if k < Z - 1:
                    gather_right(first, c, k).start()

            q = Z - 1 - k

            @pl.when((z == k) & (t - q >= 0) & (t - q < C))
            def _():
                c = t - q
                if k < Z - 1:
                    gather_left(first, c, k + 1).wait_recv()
                if k > 0:
                    gather_left(first, c, k).start()

    def outs(c, act):
        def each(half_ref, k):
            for d in (
                pltpu.make_async_copy(
                    GA.at[c, 0], half_ref.at[:, 0, k, :, pl.ds(0, LA)], out_sem.at[0, c]
                ),
                pltpu.make_async_copy(
                    GA.at[c, 1], half_ref.at[:, 1, k, :, pl.ds(0, LA)], out_sem.at[1, c]
                ),
                pltpu.make_async_copy(
                    GB.at[c], half_ref.at[:, :, k, :, pl.ds(LA, L - LA)], out_sem.at[2, c]
                ),
            ):
                act(d)

        @pl.when(c < CH)
        def _():
            each(half_up_ref, c)

        @pl.when(c >= CH)
        def _():
            each(half_down_ref, c - CH)

    def next_out(c, act):
        @pl.when(c < CH)
        def _():
            act(pltpu.make_async_copy(NX.at[c], next_up_ref.at[c], out_sem.at[3, c]))

        @pl.when(c >= CH)
        def _():
            act(pltpu.make_async_copy(NX.at[c], next_down_ref.at[c - CH], out_sem.at[3, c]))

    def lanes(x):
        s = x[:, :LANE] * x[:, :LANE]
        for i in range(1, L // LANE):
            part = x[:, i * LANE : (i + 1) * LANE]
            s = s + part * part
        return s

    def when_chunk(c):
        return pl.when((c >= 0) & (c < C))

    @pl.loop(0, C + 2 * Z)
    def _(t):
        @pl.when(t + 1 < CH)
        def _():
            load_up(t + 1).start()

        @pl.when(t < CH)
        def _():
            load_up(t).wait()
            for d in range(Z):
                for v in range(2):
                    XA[t, v, d] = stage[t % 2, d, v, :, :LA].astype(BF16)
                    XB[t, d, v] = stage[t % 2, d, v, :, LA:].astype(BF16)

        @pl.when(t < C)
        def _():
            ya(t).start()

        reduce_step(False, t)
        s = t - 1

        @when_chunk(s)
        def _():
            ya(s).wait_recv()
            for d in range(Z):
                XA[s, y, d] = (XA[s, y, d].astype(F32) + RYA[s, d].astype(F32)).astype(BF16)

        reduce_step(True, s)
        b = t - (Z - 1)

        @when_chunk(b)
        def _():
            yb(b).start()

        f = t - Z

        @pl.when(f == 0)
        def _():
            for d in load_params():
                d.wait()

        @when_chunk(f)
        def _():
            yb(f).wait_recv()
            NX[f, :, :LA] = XA[f, y, z].astype(F32) * rate
            NX[f, :, LA:] = (XB[f, z, y].astype(F32) + RYB[f].astype(F32)) * rate
            SQ[f, 0, 0] = lanes(NX[f])
            SQ[f, 0, 1] = lanes(PR[f])
            for o in range(1, m):
                sq_copy(f, o).start()

        u = t - Z

        @when_chunk(u - 1)
        def _():
            gyb_in(u - 1).wait_recv()

        gather_step(False, u - 1)
        e = u - Z

        @when_chunk(e)
        def _():
            gya_in(e).wait_recv()
            outs(e, lambda d: d.start())

        @when_chunk(u)
        def _():
            for o in range(1, m):
                sq_copy(u, o).wait_recv()
            g = SQ[u, 0, 0]
            p = SQ[u, 0, 1]
            for o in range(1, m):
                g = g + SQ[u, o, 0]
                p = p + SQ[u, o, 1]
            g = jnp.sum(g, axis=1, keepdims=True)
            p = jnp.sum(p, axis=1, keepdims=True)
            scale = learn_rate * (jnp.sqrt(p) * lax.rsqrt(g + 1e-06))
            new = PR[u] - NX[u] * scale
            NX[u] = new
            half = new.astype(BF16)
            GA[u, y, z] = half[:, :LA]
            GB[u, z, y] = half[:, LA:]
            gyb(u).start()
            next_out(u, lambda d: d.start())

        gather_step(True, u)

        @when_chunk(u - (Z - 1))
        def _():
            gya(u - (Z - 1)).start()

        for i in range(share):
            b = t * share + i

            @pl.when(b + 1 < blocks)
            def _():
                load_down(b + 1).start()

            @pl.when(b < blocks)
            def _():
                load_down(b).wait()
                turn_block(b)

    total = vec_ref[...]
    for o in range(1, n):
        vec_copy(o).wait()
        total = total + VG[o - 1]
    sums_ref[...] = total

    @pl.loop(0, C)
    def _(c):
        outs(c, lambda d: d.wait())
        next_out(c, lambda d: d.wait())
        for d in (ya(c), yb(c), gya(c), gyb(c)):
            d.wait_send()
        for o in range(1, m):
            sq_copy(c, o).wait_send()
        for k in range(Z):

            @pl.when(z == k)
            def _():
                for first in (True, False):
                    if k < Z - 1:
                        sum_right(first, c, k).wait_send()
                        gather_right(first, c, k).wait_send()
                    if k > 0:
                        sum_left(first, c, k).wait_send()
                        gather_left(first, c, k).wait_send()


def on_device(
    slope_up, slope_down, slope_norm, slope_bias, param_up, param_down, param_norm, param_bias
):
    n = lax.axis_size("batch")
    m = lax.axis_size("cols")
    Z = n // 2
    rows, L = param_up.shape
    CH = rows // R
    C = 2 * CH
    LA = max(1, round(SPLIT * L / LANE)) * LANE
    LB = L - LA
    width = slope_norm.shape[1]
    place = lax.axis_index("batch")
    up = slope_up[0].reshape(Z, 2, CH, R, L)
    down = slope_down[0]
    pup = param_up.reshape(CH, R, L)
    pdown = param_down.T.reshape(CH, R, L)
    mine = lax.dynamic_update_slice(
        jnp.zeros((2, width), F32), jnp.stack([param_norm, param_bias]), (0, place * rows)
    )
    vec = jnp.concatenate([slope_norm, slope_bias, mine], axis=0).reshape(8, width // 2)
    kinds = 12
    hbm = pl.BlockSpec(memory_space=pl.ANY)
    vmem = pl.BlockSpec(memory_space=pltpu.VMEM)
    half_up, half_down, new_up, new_down, sums = pl.pallas_call(
        functools.partial(kernel, n, m, LA),
        out_shape=(
            jax.ShapeDtypeStruct((Z, 2, CH, R, L), BF16),
            jax.ShapeDtypeStruct((Z, 2, CH, R, L), BF16),
            jax.ShapeDtypeStruct((CH, R, L), F32),
            jax.ShapeDtypeStruct((CH, R, L), F32),
            jax.ShapeDtypeStruct(vec.shape, F32),
        ),
        in_specs=[hbm, hbm, hbm, hbm, vmem],
        out_specs=(hbm, hbm, hbm, hbm, vmem),
        scratch_shapes=[
            pltpu.VMEM((2, Z, 2, R, L), F32),
            pltpu.VMEM((2, LANE, n * rows), F32),
            pltpu.VMEM((C, 2, Z, R, LA), BF16),
            pltpu.VMEM((C, Z, 2, R, LB), BF16),
            pltpu.VMEM((C, Z, R, LA), BF16),
            pltpu.VMEM((C, R, LB), BF16),
            pltpu.VMEM((C, Z + 1, R, LA), BF16),
            pltpu.VMEM((C, Z + 1, 2, R, LB), BF16),
            pltpu.VMEM((C, R, L), F32),
            pltpu.VMEM((C, R, L), F32),
            pltpu.VMEM((C, m, 2, R, LANE), F32),
            pltpu.VMEM((C, 2, Z, R, LA), BF16),
            pltpu.VMEM((C, Z, 2, R, LB), BF16),
            pltpu.VMEM((n - 1,) + vec.shape, F32),
            pltpu.SemaphoreType.DMA((2,)),
            pltpu.SemaphoreType.DMA((2,)),
            pltpu.SemaphoreType.DMA((2,)),
            pltpu.SemaphoreType.DMA((4, C)),
            pltpu.SemaphoreType.DMA((kinds, C)),
            pltpu.SemaphoreType.DMA((kinds, C)),
            pltpu.SemaphoreType.DMA((m - 1, C)),
            pltpu.SemaphoreType.DMA((m - 1, C)),
            pltpu.SemaphoreType.DMA((n - 1,)),
            pltpu.SemaphoreType.DMA((n - 1,)),
        ],
        compiler_params=pltpu.CompilerParams(
            collective_id=0, has_side_effects=True, vmem_limit_bytes=67043328
        ),
    )(up, down, pup, pdown, vec)
    half_up = half_up.reshape(n * rows, L)
    half_down = half_down.reshape(n * rows, L).T
    next_up = new_up.reshape(rows, L)
    next_down = new_down.reshape(rows, L).T
    sums = sums.reshape(4, width)
    whole = sums[2:] - learn_rate * (sums[:2] * n ** (-0.5))
    own = lax.dynamic_slice_in_dim(whole, place * rows, rows, axis=1)
    halves = whole.astype(BF16)
    return (half_up, half_down, halves[0], halves[1], next_up, next_down, own[0], own[1])


def solution(mesh):
    return jax.shard_map(
        on_device,
        mesh=mesh,
        in_specs=(
            P(("ens", "batch"), None, "cols"),
            P(("ens", "batch"), "cols", None),
            P(("ens", "batch"), None),
            P(("ens", "batch"), None),
            P(("ens", "batch"), "cols"),
            P(("ens", "cols"), "batch"),
            P(("ens", "batch")),
            P(("ens", "batch")),
        ),
        out_specs=(
            P("ens", "cols"),
            P(("ens", "cols"), None),
            P("ens"),
            P("ens"),
            P(("ens", "batch"), "cols"),
            P(("ens", "cols"), "batch"),
            P(("ens", "batch")),
            P(("ens", "batch")),
        ),
        check_vma=False,
    )
```
